512 devices in a mesh: blk: 128 (over z, y, core), col: 4 (over x).
Axes of the slice: x: 4, y: 8, z: 8, core: 2. Of those that a mesh axis runs over, the one named last changes fastest.
Arguments:
- kernel: float32 [8192, 4, 2048], P('blk', 'col'), may hold values from -8 to 60, as said below
- ritz_block: float32 [8192, 128], P(('blk', 'col')), may hold values from -0.0625 to 0.0625
- search_block: float32 [8192, 128], P(('blk', 'col')), may hold values from -0.0625 to 0.0625
- precond_diag: float32 [8192], P(('blk', 'col')), may hold values from 3 to 30
Outputs:
- new_ritz: float32 [8192, 128], P(('blk', 'col'))
- correction: float32 [8192, 128], P(('blk', 'col'))
- residual_norms: float32 [2, 128], replicated
The draws below stay inside these ranges and needn't reach their ends.
Inputs may be any that keep to these rules, and one draw needn't show every extreme that they name: kernel holds a symmetric matrix K as stated in the reference program, with a positive diagonal.
All inputs are finite; a program needn't handle non-finite values.
Results may differ from the reference program's by a relative error of at most 0.0003.
Values sent between devices are 32-bit elements; how exact they have to be, the bound alone decides.
A program may use at most 64 MiB of HBM per device.

```python
import math
import jax
import jax.numpy as jnp
from jax import lax

ROWS_DEV = 64
V = 128
ITERS = 2
N = 8192
QUARTER = 16


def draw_kernel(key, part):
    first_key, second_key = jax.random.split(jax.random.fold_in(key, 7))
    noise = jax.random.normal(first_key, (N, N), jnp.float32)
    upper_scale = 10.0
    scales = jnp.exp(jax.random.uniform(second_key, (N,), jnp.float32, 0.0, jnp.log(upper_scale)))
    roots = jnp.sqrt(scales)
    symmetric = (noise + noise.T) * (1.0 / jnp.sqrt(2.0 * N)) + 3.0 * jnp.eye(N, dtype=jnp.float32)
    matrix = symmetric * (roots[:, None] * roots[None, :])
    groups = ROWS_DEV // QUARTER
    matrix = matrix.reshape(N, N // ROWS_DEV, groups, QUARTER).transpose(0, 2, 1, 3)
    return matrix.reshape(N, groups, N // groups)


def level_of(key, shape, cuts, low, high):
    def one(dim, blocks):
        draws = jax.random.uniform(jax.random.fold_in(jax.random.fold_in(key, 6), dim), (blocks,), jnp.float32, low / len(cuts), high / len(cuts))
        return jnp.repeat(jnp.exp(draws), shape[dim] // blocks).reshape((-1,) + (1,) * (len(shape) - dim - 1))

    factor_of = one(*cuts[0])
    for cut in cuts[1:]:
        factor_of = factor_of * one(*cut)
    return factor_of


def scatter_about(stream_key, shape, deviation, bound, cuts=(), held_as=jnp.bfloat16):
    array = jax.random.normal(stream_key, shape, jnp.float32) * deviation
    if len(cuts) > 0:
        array = level_of(stream_key, shape, cuts, -0.22, 0.18) * array
    return jnp.clip(array, min=-bound, max=bound).astype(held_as)


def setup_inputs(seed: int = 0) -> dict:
    key_list = jax.random.split(jax.random.key(seed), 5)
    return {
        "kernel": draw_kernel(jax.random.fold_in(key_list[4], 71), 0),
        "ritz_block": scatter_about(key_list[1], (N, V), N ** -0.5, 0.0625, ((0, 512),), jnp.float32),
        "search_block": scatter_about(key_list[2], (N, V), N ** -0.5, 0.0625, ((0, 512),), jnp.float32),
        "precond_diag": jnp.clip(jnp.exp(math.log(30.0) - 2.3025851 * jax.random.uniform(key_list[3], (N,), jnp.float32) ** level_of(key_list[3], (N,), ((0, 512),), -0.2, 0.2)), 3.0, 30.0),
    }


highest = lax.Precision.HIGHEST

def apply_kernel(kernel, vectors):
    groups = ROWS_DEV // QUARTER
    count = vectors.shape[1]
    layout = vectors.reshape(N // ROWS_DEV, groups, QUARTER, count).transpose(1, 0, 2, 3)
    layout = layout.reshape(groups, N // groups, count)
    return jnp.einsum('iqj,qjm->im', kernel, layout, precision=highest)

def inner(former, latter):
    return lax.dot_general(former.astype(jnp.float32), latter.astype(jnp.float32), (((0,), (0,)), ((), ())), precision=highest, preferred_element_type=jnp.float32)

def coefficients(blocks, width):
    ritz_ritz, ritz_search, search_search, ritz_image, ritz_wimage, search_wimage = blocks
    metric = jnp.concatenate([jnp.concatenate([ritz_ritz, ritz_search], 1), jnp.concatenate([ritz_search.T, search_search], 1)], 0)
    projected = jnp.concatenate([jnp.concatenate([ritz_image, ritz_wimage], 1), jnp.concatenate([ritz_wimage.T, search_wimage], 1)], 0)
    lower_metric = jnp.linalg.cholesky(metric)
    halfway = lax.linalg.triangular_solve(lower_metric, projected[:, :width], left_side=True, lower=True)
    powered = lax.linalg.triangular_solve(lower_metric, halfway, left_side=True, lower=True, transpose_a=True)
    hermite = jnp.dot(powered.T, jnp.dot(metric, powered, precision=highest), precision=highest)
    lower_hermite = jnp.linalg.cholesky(hermite)
    mixing = lax.linalg.triangular_solve(lower_hermite, powered, left_side=False, lower=True, transpose_a=True)
    ritz_values = jnp.dot(mixing.T, jnp.dot(projected, mixing, precision=highest), precision=highest)
    return (mixing, ritz_values)

def update(vectors, images, search, search_images, mixing, ritz_values, precond):
    width = vectors.shape[1]
    upper_part = mixing[:width]
    lower_part = mixing[width:]
    next_ritz = jnp.dot(vectors, upper_part, precision=highest) + jnp.dot(search, lower_part, precision=highest)
    next_image = jnp.dot(images, upper_part, precision=highest) + jnp.dot(search_images, lower_part, precision=highest)
    residual = next_image - jnp.dot(next_ritz, ritz_values, precision=highest)
    squares = lax.optimization_barrier(jnp.sum(residual * residual, axis=0))
    divisor = jnp.maximum(jnp.abs(precond[:, None] - jnp.diagonal(ritz_values)[None, :]), 1.0)
    return (next_ritz, next_image, residual / divisor, squares)

def reference(kernel, ritz_block, search_block, precond_diag):
    width = ritz_block.shape[1]
    vectors = ritz_block
    search = search_block
    images = apply_kernel(kernel, vectors)
    search_images = apply_kernel(kernel, search)
    norm_rows = []
    for iteration in range(ITERS):
        if iteration > 0:
            search_images = apply_kernel(kernel, search)
        blocks = (inner(vectors, vectors), inner(vectors, search), inner(search, search), inner(vectors, images), inner(vectors, search_images), inner(search, search_images))
        mixing, ritz_values = coefficients(blocks, width)
        vectors, images, search, squares = update(vectors, images, search, search_images, mixing, ritz_values, precond_diag)
        norm_rows.append(jnp.sqrt(squares))
    return (vectors, search, jnp.stack(norm_rows, 0))
```

```python
import functools

import jax
import jax.numpy as jnp
from jax import lax
from jax.experimental import pallas as pl
from jax.experimental.pallas import tpu as pltpu
from jax.sharding import Mesh
from jax.sharding import PartitionSpec as P

MESH = pl.DeviceIdType.MESH
BLK = ("blk_0", "blk_1", "blk_2")
BLK_COL = ("blk_0", "blk_1", "blk_2", "col")
V = 128
Q = 16
PANEL = 16
f32 = jnp.float32
bf16 = jnp.bfloat16
highest = lax.Precision.HIGHEST


def dot(a, b, ca=1, cb=0):
    return lax.dot_general(
        a, b, (((ca,), (cb,)), ((), ())), precision=highest, preferred_element_type=f32
    )


def split(a):
    high = a.astype(bf16)
    return high, (a - high.astype(f32)).astype(bf16)


def dot3(a, b, ca=1, cb=0):
    dims = (((ca,), (cb,)), ((), ()))

    def one(x, y):
        return lax.dot_general(x, y, dims, preferred_element_type=f32)

    return one(a[0], b[0]) + (one(a[0], b[1]) + one(a[1], b[0]))


def inverse_factor(matrix, work):
    row = lax.broadcasted_iota(jnp.int32, (V, V), 0)
    lane = lax.broadcasted_iota(jnp.int32, (V, V), 1)
    work[:, :V] = matrix
    work[:, V:] = jnp.where(row == lane, 1.0, 0.0).astype(f32)
    sub = lax.broadcasted_iota(jnp.int32, (PANEL, V), 0)
    for start in range(0, V, PANEL):
        end = start + PANEL
        left = work[start:end, :V]
        right = work[start:end, V:]
        columns = [
            jnp.broadcast_to(left[:, start + t : start + t + 1], (PANEL, V)) for t in range(PANEL)
        ]
        scale = jnp.zeros((PANEL, V), f32)
        for r in range(PANEL):
            inverse = lax.rsqrt(jnp.broadcast_to(columns[r][r : r + 1, :], (PANEL, V)))
            scale = jnp.where(sub == r, inverse, scale)
            if r == PANEL - 1:
                break
            factor = jnp.where(sub > r, columns[r] * inverse, 0.0)
            for t in range(r + 1, PANEL):
                columns[t] = columns[t] - factor * factor[t : t + 1, :]
            factor = factor * inverse
            left = left - factor * left[r : r + 1, :]
            right = right - factor * right[r : r + 1, :]
        left = left * scale
        right = right * scale
        work[start:end, V:] = right
        if end < V:
            lower = dot(left, jnp.concatenate([left, right], 1), 0, 0)
            work[end:, :] = work[end:, :] - lower[end:, :]
    return work[:, V:]


def mixing_of(blocks, work, first):
    ritz_ritz, ritz_search, search_search, ritz_image, cross_image, search_image = blocks
    if first:
        top = inverse_factor(ritz_ritz, work)
        side = dot(top, ritz_search)
    else:
        side = ritz_search
    low = inverse_factor(search_search - dot(side, side, 0, 0), work)
    upper = dot(top, ritz_image) if first else ritz_image
    lower = dot(low, cross_image - dot(side, upper, 0, 0), 1, 0)
    back = inverse_factor(dot(upper, upper, 0, 0) + dot(lower, lower, 0, 0), work)
    upper = dot(upper, back, 1, 1)
    lower = dot(lower, back, 1, 1)
    lower = dot(low, lower, 0, 0)
    upper = upper - dot(side, lower)
    if first:
        upper = dot(top, upper, 0, 0)
    return upper, lower


def coefficients_kernel(first, *refs):
    *ins, mix_ref, ritz_ref, work = refs
    if first:
        metric, projected = ins
        xx, xw, ww = (metric[i * V : (i + 1) * V, :] for i in range(3))
        gxx, gxw, gww = (projected[i * V : (i + 1) * V, :] for i in range(3))
    else:
        sums, last, ritz = ins
        xx = None
        xw, ww, gxw = (sums[i * V : (i + 1) * V, :] for i in range(3))
        gww = last[...]
        gxx = ritz[...]
    upper, lower = mixing_of((xx, xw, ww, gxx, gxw.T, gww), work, first)
    mix_ref[:V, :] = upper
    mix_ref[V:, :] = lower
    one = dot(gxx, upper) + dot(gxw, lower)
    two = dot(gxw, upper, 0, 0) + dot(gww, lower)
    ritz_ref[...] = dot(upper, one, 0, 0) + dot(lower, two, 0, 0)


def coefficients(first, *operands):
    return pl.pallas_call(
        functools.partial(coefficients_kernel, first),
        out_shape=(
            jax.ShapeDtypeStruct((2 * V, V), f32),
            jax.ShapeDtypeStruct((V, V), f32),
        ),
        in_specs=[pl.BlockSpec(memory_space=pltpu.VMEM)] * len(operands),
        out_specs=(pl.BlockSpec(memory_space=pltpu.VMEM),) * 2,
        scratch_shapes=[pltpu.VMEM((V, 2 * V), f32)],
    )(*operands)


class Place:
    def __init__(self, dims):
        self.dims = dims
        self.z, self.y, self.core, self.x = (lax.axis_index(a) for a in BLK_COL)

    def plane(self, axis, step):
        name = ("blk_0", "blk_1")[axis]
        size = self.dims[axis]
        here = (self.z, self.y)[axis]
        return {name: lax.rem(here + step + size, size)}

    def near(self, index):
        dx, dc = index // 2, index % 2
        x = lax.rem(self.x + dx, self.dims[3])
        core = lax.rem(self.core + dc, 2)
        return x, core, {"col": x, "blk_2": core}

    def group(self):
        return self.x * 2 + self.core

    def enter(self, plane):
        barrier = pltpu.get_barrier_semaphore()
        count = 0
        peers = [self.near(i)[2] for i in range(1, 2 * self.dims[3])]
        if plane:
            for axis in range(2):
                peers += [self.plane(axis, s) for s in range(1, self.dims[axis])]
        for peer in peers:
            pl.semaphore_signal(barrier, inc=1, device_id=peer, device_id_type=MESH)
            count += 1
        return barrier, count


def remote(src, dst, send, recv, to):
    return pltpu.make_async_remote_copy(
        src_ref=src,
        dst_ref=dst,
        send_sem=send,
        recv_sem=recv,
        device_id=to,
        device_id_type=MESH,
    )


class Flow:
    def __init__(self, place, buffer, rows, first, sems):
        self.place, self.buffer, self.rows, self.first = place, buffer, rows, first
        self.second = 1 - first
        self.sems = sems
        self.at = 0
        self.sent = []

    def sem(self):
        self.at += 1
        return self.sems.at[0, self.at - 1], self.sems.at[1, self.at - 1]

    def view(self, z, y):
        return self.buffer.at[z, y, self.rows]

    def begin(self):
        p = self.place
        self.own = []
        for step in range(1, p.dims[self.first]):
            ref = self.view(p.z, p.y)
            copy = remote(ref, ref, *self.sem(), p.plane(self.first, step))
            copy.start()
            self.own.append(copy)

    def middle(self):
        for copy in self.own:
            copy.wait_recv()
        self.sent += self.own
        self.moving = {}
        for chunk in range(2):
            for way in (1, -1):
                self.forward(way, chunk, 0)

    def line(self, origin, chunk):
        half = self.place.dims[self.first] // 2
        part = pl.ds(chunk * half, half)
        if self.first == 0:
            return self.buffer.at[part, origin, self.rows]
        return self.buffer.at[origin, part, self.rows]

    def last(self, way, chunk, hop):
        return hop == self.place.dims[self.second] // 2 - 1 and (way == 1) != (chunk == 0)

    def forward(self, way, chunk, hop):
        p = self.place
        size = p.dims[self.second]
        if hop >= size // 2 or self.last(way, chunk, hop):
            return
        here = (p.z, p.y)[self.second]
        ref = self.line(lax.rem(here - way * hop + size, size), chunk)
        copy = remote(ref, ref, *self.sem(), p.plane(self.second, way))
        copy.start()
        self.moving[way, chunk, hop] = copy

    def relay(self, hop):
        for chunk in range(2):
            for way in (1, -1):
                copy = self.moving.get((way, chunk, hop))
                if copy is not None:
                    copy.wait_recv()
                    self.sent.append(copy)
                    self.forward(way, chunk, hop + 1)

    @staticmethod
    def finish(flows):
        for flow in flows:
            flow.middle()
        for hop in range(max(f.place.dims[f.second] // 2 for f in flows)):
            for flow in flows:
                flow.relay(hop)

    @staticmethod
    def drain(flows):
        for flow in flows:
            for copy in flow.sent:
                copy.wait_send()


def flow_sems():
    return pltpu.SemaphoreType.DMA((2, 24))


class Spread:
    def __init__(self, place, source, target, sems):
        self.place = place
        self.copies = []
        for i in range(1, 2 * place.dims[3]):
            x, core, to = place.near(i)
            self.copies.append(
                remote(source(x, core), target(i), sems.at[0, i], sems.at[1, i], to)
            )
        for copy in self.copies:
            copy.start()

    def arrive(self):
        for copy in self.copies:
            copy.wait_recv()

    def drain(self):
        for copy in self.copies:
            copy.wait_send()


class Sum:
    def __init__(self, place, value, pieces, landed, whole, sems):
        self.place, self.pieces, self.landed, self.whole = place, pieces, landed, whole
        self.sems = sems
        pieces[...] = value.reshape(pieces.shape)
        self.scatter = Spread(
            place, lambda x, core: pieces.at[x * 2 + core], lambda i: landed.at[i], sems.at[0]
        )

    def middle(self):
        place, own = self.place, self.place.group()
        self.scatter.arrive()
        total = self.pieces[own]
        for i in range(1, 2 * place.dims[3]):
            total = total + self.landed[i]
        self.whole[own] = total
        self.share = Spread(
            place,
            lambda x, core: self.whole.at[own],
            lambda i: self.whole.at[own],
            self.sems.at[1],
        )

    def arrive(self):
        self.share.arrive()

    def drain(self):
        self.scatter.drain()
        self.share.drain()


def near_sems(*lead):
    return pltpu.SemaphoreType.DMA((*lead, 2, 8))


def sum_scratch(group, rows):
    return [pltpu.VMEM((group, rows, V), f32)] * 3 + [near_sems(2)]


def rows_of(buffer):
    return buffer[...].reshape(-1, buffer.shape[-1])


def images_kernel(
    dims, k_in, x_in, w_in, d_in, metric, projected, yx, yw, zx, zw, kern, diag,
    gx, gw, hx, hw, gd, kraw, kown, kland, part, landed,
    m0, m1, m2, msem, p0, p1, p2, psem,
    load, ksem, sx, sw, tx, tw, sd, rs,
):
    place = Place(dims)
    nz, ny, _, nx = dims
    group = 2 * nx
    barrier, count = place.enter(True)
    loads = [
        pltpu.make_async_copy(x_in, gx.at[place.z, place.y], load.at[0]),
        pltpu.make_async_copy(w_in, gw.at[place.z, place.y], load.at[1]),
        pltpu.make_async_copy(d_in, gd.at[place.z, place.y], load.at[2]),
        pltpu.make_async_copy(k_in, kraw, load.at[3]),
    ]
    for copy in loads:
        copy.start()
    for copy in loads[:3]:
        copy.wait()
    pl.semaphore_wait(barrier, count)
    flows = [
        Flow(place, gx, slice(None), 1, sx),
        Flow(place, gw, slice(None), 0, sw),
    ]
    for flow in flows:
        flow.begin()
    small = Flow(place, gd, slice(None), 1, sd)
    small.begin()
    loads[3].wait()
    i = lax.broadcasted_iota(jnp.int32, (2 * V, 2 * V), 0)
    j = lax.broadcasted_iota(jnp.int32, (2 * V, 2 * V), 1)
    to = ((i // Q) % 2) * V + (i // (2 * Q)) * Q + i % Q
    mover = jnp.where(j == to, 1.0, 0.0).astype(f32)
    for tile in range(kraw.shape[1] // (2 * V)):
        moved = dot(kraw[:, tile * 2 * V : (tile + 1) * 2 * V], mover)
        kown[0, :, tile * V : (tile + 1) * V] = moved[:, :V]
        kown[1, :, tile * V : (tile + 1) * V] = moved[:, V:]
    swap = remote(kown.at[1 - place.core], kland, ksem.at[0], ksem.at[1], place.near(1)[2])
    swap.start()
    Flow.finish(flows + [small])
    swap.wait()
    mine, other = kown[place.core], kland[...]
    kern[0] = mine
    kern[1] = other
    both = split(jnp.concatenate([mine, other], 0))
    y = jnp.concatenate([rows_of(gx), rows_of(gw)], 1)
    ys = split(y)
    image = dot3(both, ys)
    rows = mine.shape[0]
    part[place.core] = image[:rows].reshape(nx, Q, 2 * V)
    part[1 - place.core] = image[rows:].reshape(nx, Q, 2 * V)
    scatter = Spread(place, lambda x, core: part.at[core, x], lambda i: landed.at[i], rs)
    gram = dot3(ys, ys, 0, 0)
    gram = jnp.concatenate([gram[:V, :V], gram[:V, V:], gram[V:, V:]], 0)
    sums = Sum(place, gram, m0, m1, m2, msem)
    scatter.arrive()
    total = part[place.core, place.x]
    for i in range(1, group):
        total = total + landed[i]
    hx[place.z, place.y] = total[:, :V]
    hw[place.z, place.y] = total[:, V:]
    again = [
        Flow(place, hx, slice(None), 1, tx),
        Flow(place, hw, slice(None), 0, tw),
    ]
    for flow in again:
        flow.begin()
    height = nz * ny * Q
    r = lax.broadcasted_iota(jnp.int32, (height, nz * ny), 0)
    b = lax.broadcasted_iota(jnp.int32, (height, nz * ny), 1)
    pick = jnp.where(r // Q == b, 1.0, 0.0).astype(f32)
    entries = dot(pick, gd[...].reshape(nz * ny, V))
    r = lax.broadcasted_iota(jnp.int32, (height, V), 0)
    b = lax.broadcasted_iota(jnp.int32, (height, V), 1)
    entries = jnp.where(r % Q == b, entries, 0.0)
    diag[...] = dot(entries, jnp.ones((V, V), f32))
    yx[...] = y[:, :V]
    yw[...] = y[:, V:]
    sums.middle()
    Flow.finish(again)
    sums.arrive()
    metric[...] = rows_of(m2)
    z = jnp.concatenate([rows_of(hx), rows_of(hw)], 1)
    zx[...] = z[:, :V]
    zw[...] = z[:, V:]
    gram = dot3(ys, split(z), 0, 0)
    gram = jnp.concatenate([gram[:V, :V], gram[:V, V:], gram[V:, V:]], 0)
    more = Sum(place, gram, p0, p1, p2, psem)
    more.middle()
    more.arrive()
    projected[...] = rows_of(p2)
    Flow.drain(flows + [small] + again)
    scatter.drain()
    sums.drain()
    more.drain()


def moved_on(x, w, kx, kw, mix, ritz, diag, norm_only=False):
    eye = jnp.where(
        lax.broadcasted_iota(jnp.int32, (V, V), 0) == lax.broadcasted_iota(jnp.int32, (V, V), 1),
        ritz,
        0.0,
    )
    values = jnp.sum(eye, axis=0, keepdims=True)
    upper, lower = split(mix[:V]), split(mix[V:])
    vectors = dot3(split(x), upper) + dot3(split(w), lower)
    images = dot3(split(kx), upper) + dot3(split(kw), lower)
    residual = images - dot3(split(vectors), split(ritz))
    squares = jnp.sum(residual * residual, axis=0, keepdims=True)
    search = residual / jnp.maximum(jnp.abs(diag - values), 1.0)
    return vectors, images, search, squares


def search_kernel(
    dims, yx, yw, zx, zw, kern, diag, mix, ritz, sums_out, last_out, norm, nx_out, nk_out, nw_out, hk_out,
    part, landed, hk, q0, q1, q2, qsem, l0, l1, l2, lsem, nsum, nland,
    tx, tw, rs, ns,
):
    place = Place(dims)
    group = 2 * dims[3]
    barrier, count = place.enter(True)
    vectors, images, search, squares = moved_on(
        yx[...], yw[...], zx[...], zw[...], mix[...], ritz[...], diag[...]
    )
    ws = split(search)
    rows = kern.shape[1]
    image = dot3(split(kern[...].reshape(2 * rows, -1)), ws)
    part[place.core] = image[:rows].reshape(dims[3], Q, V)
    part[1 - place.core] = image[rows:].reshape(dims[3], Q, V)
    nsum[...] = jnp.broadcast_to(squares, (8, V))
    pl.semaphore_wait(barrier, count)
    scatter = Spread(place, lambda x, core: part.at[core, x], lambda i: landed.at[i], rs)
    left = jnp.concatenate([vectors, search, images], 1)
    sums = Sum(place, dot3(split(left), ws, 0, 0), q0, q1, q2, qsem)
    norms = Spread(place, lambda x, core: nsum, lambda i: nland.at[i], ns)
    scatter.arrive()
    total = part[place.core, place.x]
    for i in range(1, group):
        total = total + landed[i]
    hk[place.z, place.y] = total
    flows = [
        Flow(place, hk, slice(0, Q // 2), 1, tx),
        Flow(place, hk, slice(Q // 2, Q), 0, tw),
    ]
    for flow in flows:
        flow.begin()
    nx_out[...] = vectors
    nk_out[...] = images
    nw_out[...] = search
    sums.middle()
    Flow.finish(flows)
    sums.arrive()
    sums_out[...] = rows_of(q2)
    norms.arrive()
    squares = nsum[...]
    for i in range(1, group):
        squares = squares + nland[i]
    norm[...] = jnp.sqrt(squares)
    final = rows_of(hk)
    hk_out[...] = final
    more = Sum(place, dot3(ws, split(final), 0, 0), l0, l1, l2, lsem)
    more.middle()
    more.arrive()
    last_out[...] = rows_of(l2)
    Flow.drain(flows)
    scatter.drain()
    sums.drain()
    norms.drain()
    more.drain()


def final_kernel(
    dims, yx, yw, zx, zw, diag, mix, ritz, norm_in, ritz_out, search_out, norms_out,
    xs, ss, nsum, nland, ns,
):
    place = Place(dims)
    barrier, count = place.enter(False)
    vectors, _, search, squares = moved_on(
        yx[...], yw[...], zx[...], zw[...], mix[...], ritz[...], diag[...]
    )
    nsum[...] = jnp.broadcast_to(squares, (8, V))
    pl.semaphore_wait(barrier, count)
    norms = Spread(place, lambda x, core: nsum, lambda i: nland.at[i], ns)
    xs[...] = vectors
    ss[...] = search
    own = pl.ds(pl.multiple_of((place.z * dims[1] + place.y) * Q, Q), Q)
    ritz_out[...] = xs[own, :]
    search_out[...] = ss[own, :]
    norms.arrive()
    squares = nsum[...]
    for i in range(1, 2 * dims[3]):
        squares = squares + nland[i]
    norms_out[0:1, :] = norm_in[0:1, :]
    norms_out[1:2, :] = jnp.sqrt(squares)[0:1, :]
    norms.drain()


def vmem(count):
    return [pl.BlockSpec(memory_space=pltpu.VMEM)] * count


def shapes(*sizes):
    return tuple(jax.ShapeDtypeStruct(s, f32) for s in sizes)


def communicating(body, dims, number, in_specs, outs, scratch):
    return pl.pallas_call(
        functools.partial(body, dims),
        out_shape=outs,
        in_specs=in_specs,
        out_specs=tuple(vmem(len(outs))),
        scratch_shapes=scratch,
        compiler_params=pltpu.CompilerParams(collective_id=number, has_side_effects=True),
    )


def per_device(dims, kernel, ritz_block, search_block, precond_diag):
    nz, ny, _, nx = dims
    height, group, rows = nz * ny * Q, 2 * nx, nx * Q
    tall = (height, V)
    grid = pltpu.VMEM((nz, ny, Q, V), f32)
    entries = jnp.pad(precond_diag, (0, V - Q)).reshape(1, V)
    metric, projected, yx, yw, zx, zw, kern, diag = communicating(
        images_kernel,
        dims,
        0,
        [pl.BlockSpec(memory_space=pl.ANY)] * 4,
        shapes((3 * V, V), (3 * V, V), tall, tall, tall, tall, (2, rows, height), tall),
        [grid] * 4
        + [
            pltpu.VMEM((nz, ny, 1, V), f32),
            pltpu.VMEM((rows, 2 * height), f32),
            pltpu.VMEM((2, rows, height), f32),
            pltpu.VMEM((rows, height), f32),
            pltpu.VMEM((2, nx, Q, 2 * V), f32),
            pltpu.VMEM((group, Q, 2 * V), f32),
        ]
        + sum_scratch(group, 3 * V // group) * 2
        + [pltpu.SemaphoreType.DMA((4,)), pltpu.SemaphoreType.DMA((2,))]
        + [flow_sems() for _ in range(5)]
        + [near_sems()],
    )(kernel.reshape(rows, 2 * height), ritz_block, search_block, entries)
    mix, ritz = coefficients(True, metric, projected)
    sums, last, norm, xx, kx, ww, kw = communicating(
        search_kernel,
        dims,
        1,
        vmem(8),
        shapes((3 * V, V), (V, V), (8, V), tall, tall, tall, tall),
        [
            pltpu.VMEM((2, nx, Q, V), f32),
            pltpu.VMEM((group, Q, V), f32),
            grid,
        ]
        + sum_scratch(group, 3 * V // group)
        + sum_scratch(group, V // group)
        + [
            pltpu.VMEM((8, V), f32),
            pltpu.VMEM((group, 8, V), f32),
        ]
        + [flow_sems() for _ in range(2)]
        + [near_sems() for _ in range(2)],
    )(yx, yw, zx, zw, kern, diag, mix, ritz)
    mix, ritz = coefficients(False, sums, last, ritz)
    return communicating(
        final_kernel,
        dims,
        2,
        vmem(8),
        shapes((Q, V), (Q, V), (2, V)),
        [
            pltpu.VMEM(tall, f32),
            pltpu.VMEM(tall, f32),
            pltpu.VMEM((8, V), f32),
            pltpu.VMEM((group, 8, V), f32),
            near_sems(),
        ],
    )(xx, ww, kx, kw, diag, mix, ritz, norm)


def solution(mesh):
    chips, cols = mesh.shape["blk"] // 2, mesh.shape["col"]
    ny = min(8, chips // 2)
    dims = (chips // ny, ny, 2, cols)
    torus = Mesh(mesh.devices.reshape(dims), BLK_COL)
    placed = (P(BLK, "col", None), P(BLK_COL, None), P(BLK_COL, None), P(BLK_COL))
    return jax.shard_map(
        functools.partial(per_device, dims),
        mesh=torus,
        in_specs=placed,
        out_specs=(P(BLK_COL, None), P(BLK_COL, None), P()),
        check_vma=False,
    )
```

```python
import functools

import jax
import jax.numpy as jnp
from jax import lax
from jax.experimental import pallas as pl
from jax.experimental.pallas import tpu as pltpu
from jax.sharding import Mesh
from jax.sharding import PartitionSpec as P

MESH = pl.DeviceIdType.MESH
BLK = ("blk_0", "blk_1", "blk_2")
BLK_COL = ("blk_0", "blk_1", "blk_2", "col")
V = 128
Q = 16
PANEL = 16
f32 = jnp.float32
bf16 = jnp.bfloat16
highest = lax.Precision.HIGHEST


def dot(a, b, ca=1, cb=0):
    return lax.dot_general(
        a, b, (((ca,), (cb,)), ((), ())), precision=highest, preferred_element_type=f32
    )


def split(a):
    high = a.astype(bf16)
    return high, (a - high.astype(f32)).astype(bf16)


def dot3(a, b, ca=1, cb=0):
    dims = (((ca,), (cb,)), ((), ()))

    def one(x, y):
        return lax.dot_general(x, y, dims, preferred_element_type=f32)

    return one(a[0], b[0]) + (one(a[0], b[1]) + one(a[1], b[0]))


def inverse_factor(matrix, work):
    row = lax.broadcasted_iota(jnp.int32, (V, V), 0)
    lane = lax.broadcasted_iota(jnp.int32, (V, V), 1)
    work[:, :V] = matrix
    work[:, V:] = jnp.where(row == lane, 1.0, 0.0).astype(f32)
    sub = lax.broadcasted_iota(jnp.int32, (PANEL, V), 0)
    for start in range(0, V, PANEL):
        end = start + PANEL
        left = work[start:end, :V]
        right = work[start:end, V:]
        columns = [
            jnp.broadcast_to(left[:, start + t : start + t + 1], (PANEL, V)) for t in range(PANEL)
        ]
        scale = jnp.zeros((PANEL, V), f32)
        for r in range(PANEL):
            inverse = lax.rsqrt(jnp.broadcast_to(columns[r][r : r + 1, :], (PANEL, V)))
            scale = jnp.where(sub == r, inverse, scale)
            if r == PANEL - 1:
                break
            factor = jnp.where(sub > r, columns[r] * inverse, 0.0)
            for t in range(r + 1, PANEL):
                columns[t] = columns[t] - factor * factor[t : t + 1, :]
            factor = factor * inverse
            left = left - factor * left[r : r + 1, :]
            right = right - factor * right[r : r + 1, :]
        left = left * scale
        right = right * scale
        work[start:end, V:] = right
        if end < V:
            lower = dot(left, jnp.concatenate([left, right], 1), 0, 0)
            work[end:, :] = work[end:, :] - lower[end:, :]
    return work[:, V:]


class Place:
    def __init__(self, dims):
        self.dims = dims
        self.z, self.y, self.core, self.x = (lax.axis_index(a) for a in BLK_COL)

    def plane(self, axis, step):
        name = ("blk_0", "blk_1")[axis]
        size = self.dims[axis]
        here = (self.z, self.y)[axis]
        return {name: lax.rem(here + step + size, size)}

    def near(self, index):
        dx, dc = index // 2, index % 2
        x = lax.rem(self.x + dx, self.dims[3])
        core = lax.rem(self.core + dc, 2)
        return x, core, {"col": x, "blk_2": core}

    def group(self):
        return self.x * 2 + self.core

    def enter(self, plane):
        barrier = pltpu.get_barrier_semaphore()
        count = 0
        peers = [self.near(i)[2] for i in range(1, 2 * self.dims[3])]
        if plane:
            for axis in range(2):
                peers += [self.plane(axis, s) for s in range(1, self.dims[axis])]
        for peer in peers:
            pl.semaphore_signal(barrier, inc=1, device_id=peer, device_id_type=MESH)
            count += 1
        return barrier, count


def remote(src, dst, send, recv, to):
    return pltpu.make_async_remote_copy(
        src_ref=src,
        dst_ref=dst,
        send_sem=send,
        recv_sem=recv,
        device_id=to,
        device_id_type=MESH,
    )


class Flow:
    def __init__(self, place, buffer, rows, first, sems):
        self.place, self.buffer, self.rows, self.first = place, buffer, rows, first
        self.second = 1 - first
        self.near = Flow.steps(place.dims[first])
        self.far = Flow.steps(place.dims[self.second])[::-1]
        self.send, self.receive = sems
        self.sent = []
        here = (place.z, place.y)
        self.here, self.there = here[first], here[self.second]

    @staticmethod
    def steps(size):
        return sorted((d if d <= size // 2 else d - size for d in range(1, size)), key=abs)

    def start(self, ref, number, axis, step):
        copy = remote(
            ref,
            ref,
            self.send.at[len(self.sent)],
            self.receive.at[number],
            self.place.plane(axis, step),
        )
        copy.start()
        self.sent.append(copy)
        return copy

    def block(self, here, there):
        at = (here, there) if self.first == 0 else (there, here)
        return self.buffer.at[at[0], at[1], self.rows]

    def fan(self, here):
        for i, step in enumerate(self.far):
            self.start(self.block(here, self.there), len(self.near) + i, self.second, step)

    def begin(self):
        own = self.block(self.here, self.there)
        self.first_copies = [
            self.start(own, i, self.first, step) for i, step in enumerate(self.near)
        ]
        self.fan(self.here)

    def relay(self, i):
        self.first_copies[i].wait_recv()
        size = self.place.dims[self.first]
        self.fan(lax.rem(self.here - self.near[i] + size, size))

    def end(self):
        size = self.place.dims[self.second]
        for i, step in enumerate(self.far):
            origin = lax.rem(self.there - step + size, size)
            if self.first == 0:
                line = self.buffer.at[:, origin, self.rows]
            else:
                line = self.buffer.at[origin, :, self.rows]
            number = len(self.near) + i
            remote(
                line,
                line,
                self.send.at[0],
                self.receive.at[number],
                self.place.plane(self.second, step),
            ).wait_recv()

    @staticmethod
    def relays(flows):
        for i in range(max(len(f.near) for f in flows)):
            for flow in flows:
                if i < len(flow.near):
                    flow.relay(i)

    @staticmethod
    def ends(flows):
        for flow in flows:
            flow.end()

    @staticmethod
    def drain(flows):
        for flow in flows:
            for copy in flow.sent:
                copy.wait_send()


def flow_sems(dims):
    nz, ny = dims[:2]
    return [
        pltpu.SemaphoreType.DMA((nz * ny + max(nz, ny),)),
        pltpu.SemaphoreType.DMA((nz + ny,)),
    ]


class Spread:
    def __init__(self, place, source, target, sems):
        self.place = place
        self.copies = []
        for i in range(1, 2 * place.dims[3]):
            x, core, to = place.near(i)
            self.copies.append(
                remote(source(x, core), target(i), sems.at[0, i], sems.at[1, i], to)
            )
        for copy in self.copies:
            copy.start()

    def arrive(self):
        for copy in self.copies:
            copy.wait_recv()

    def drain(self):
        for copy in self.copies:
            copy.wait_send()


class Sum:
    def __init__(self, place, value, pieces, landed, whole, sems):
        self.place, self.pieces, self.landed, self.whole = place, pieces, landed, whole
        self.sems = sems
        pieces[...] = value.reshape(pieces.shape)
        self.scatter = Spread(
            place, lambda x, core: pieces.at[x * 2 + core], lambda i: landed.at[i], sems.at[0]
        )

    def middle(self):
        place, own = self.place, self.place.group()
        self.scatter.arrive()
        total = self.pieces[own]
        for i in range(1, 2 * place.dims[3]):
            total = total + self.landed[i]
        self.whole[own] = total
        self.share = Spread(
            place,
            lambda x, core: self.whole.at[own],
            lambda i: self.whole.at[own],
            self.sems.at[1],
        )

    def arrive(self):
        self.share.arrive()

    def drain(self):
        self.scatter.drain()
        self.share.drain()


def near_sems(*lead):
    return pltpu.SemaphoreType.DMA((*lead, 2, 8))


def sum_scratch(group, rows):
    return [pltpu.VMEM((group, rows, V), f32)] * 3 + [near_sems(2)]


def rows_of(buffer):
    return buffer[...].reshape(-1, buffer.shape[-1])


def three(gram):
    return jnp.concatenate([gram[:V, :V], gram[:V, V:], gram[V:, V:]], 0)


def metric_factor(metric, work):
    xx, xw, ww = (metric[i * V : (i + 1) * V, :] for i in range(3))
    top = inverse_factor(xx, work)
    side = dot(top, xw)
    low = inverse_factor(ww - dot(side, side, 0, 0), work)
    cross = -dot(dot(low, side, 1, 1), top)
    zero = jnp.zeros((V, V), f32)
    return jnp.concatenate(
        [jnp.concatenate([top, zero], 1), jnp.concatenate([cross, low], 1)], 0
    )


def first_mixing(factor, projected, work):
    xx, xw, ww = (projected[i * V : (i + 1) * V, :] for i in range(3))
    left = jnp.concatenate([xx, xw.T], 0)
    whole = jnp.concatenate([left, jnp.concatenate([xw, ww], 0)], 1)
    half = dot(factor, left)
    power = dot(factor, half, 0, 0)
    applied = dot(whole, power)
    back = inverse_factor(dot(half, half, 0, 0), work)
    mix = dot(power, back, 1, 1)
    return mix, dot(mix, dot(applied, back, 1, 1), 0, 0)


def second_mixing(sums, ritz, work):
    xw, ww, image = (sums[i * V : (i + 1) * V, :] for i in range(3))
    low = inverse_factor(ww - dot(xw, xw, 0, 0), work)
    lower = dot(low, image.T - dot(xw, ritz, 0, 0))
    back = inverse_factor(dot(ritz, ritz, 0, 0) + dot(lower, lower, 0, 0), work)
    lower = dot(low, dot(lower, back, 1, 1), 0, 0)
    upper = dot(ritz, back, 1, 1) - dot(xw, lower)
    return jnp.concatenate([upper, lower], 0)


def correction_of(images, vectors, ritz, diag):
    row = lax.broadcasted_iota(jnp.int32, (V, V), 0)
    lane = lax.broadcasted_iota(jnp.int32, (V, V), 1)
    values = jnp.sum(jnp.where(row == lane, ritz, 0.0), axis=0, keepdims=True)
    residual = images - dot3(vectors, split(ritz))
    squares = jnp.sum(residual * residual, axis=0, keepdims=True)
    return residual / jnp.maximum(jnp.abs(diag - values), 1.0), squares


def davidson_kernel(
    dims, k_in, x_in, w_in, d_in, ritz_out, search_out, norms_out,
    gx, gw, hx, hw, hk, gd, entry, kraw, kown, kland, part, landed, less, lessland,
    m0, m1, m2, msem, p0, p1, p2, psem, q0, q1, q2, qsem, l0, l1, l2, lsem,
    nsum, nland, osum, oland, xs, ss, work,
    load, ksem, ax, bx, aw, bw, cx, dx, cw, dw, ek, fk, gk, ik, ad, bd, rs, ts, ns, os,
):
    place = Place(dims)
    nz, ny, _, nx = dims
    group = 2 * nx
    barrier, count = place.enter(True)
    loads = [
        pltpu.make_async_copy(x_in, gx.at[place.z, place.y], load.at[0]),
        pltpu.make_async_copy(w_in, gw.at[place.z, place.y], load.at[1]),
        pltpu.make_async_copy(d_in, gd.at[place.z, place.y], load.at[2]),
        pltpu.make_async_copy(k_in, kraw, load.at[3]),
    ]
    for copy in loads:
        copy.start()
    for copy in loads[:3]:
        copy.wait()
    pl.semaphore_wait(barrier, count)
    flows = [
        Flow(place, gx, slice(None), 1, (ax, bx)),
        Flow(place, gw, slice(None), 0, (aw, bw)),
    ]
    for flow in flows:
        flow.begin()
    Flow.relays(flows)
    small = Flow(place, gd, slice(None), 1, (ad, bd))
    small.begin()
    loads[3].wait()
    i = lax.broadcasted_iota(jnp.int32, (2 * V, 2 * V), 0)
    j = lax.broadcasted_iota(jnp.int32, (2 * V, 2 * V), 1)
    to = ((i // Q) % 2) * V + (i // (2 * Q)) * Q + i % Q
    mover = jnp.where(j == to, 1.0, 0.0).astype(f32)
    for tile in range(kraw.shape[1] // (2 * V)):
        moved = dot(kraw[:, tile * 2 * V : (tile + 1) * 2 * V], mover)
        kown[0, :, tile * V : (tile + 1) * V] = moved[:, :V]
        kown[1, :, tile * V : (tile + 1) * V] = moved[:, V:]
    swap = remote(kown.at[1 - place.core], kland, ksem.at[0], ksem.at[1], place.near(1)[2])
    swap.start()
    Flow.relays([small])
    swap.wait()
    both = split(jnp.concatenate([kown[place.core], kland[...]], 0))
    rows = kland.shape[0]
    Flow.ends(flows)
    ys = split(jnp.concatenate([rows_of(gx), rows_of(gw)], 1))
    image = dot3(both, ys)
    part[place.core] = image[:rows].reshape(nx, Q, 2 * V)
    part[1 - place.core] = image[rows:].reshape(nx, Q, 2 * V)
    scatter = Spread(place, lambda x, core: part.at[core, x], lambda i: landed.at[i], rs)
    sums = Sum(place, three(dot3(ys, ys, 0, 0)), m0, m1, m2, msem)
    scatter.arrive()
    total = part[place.core, place.x]
    for i in range(1, group):
        total = total + landed[i]
    hx[place.z, place.y] = total[:, :V]
    hw[place.z, place.y] = total[:, V:]
    again = [
        Flow(place, hx, slice(None), 1, (cx, dx)),
        Flow(place, hw, slice(None), 0, (cw, dw)),
    ]
    for flow in again:
        flow.begin()
    sums.middle()
    Flow.relays(again)
    small.end()
    height = nz * ny * Q
    r = lax.broadcasted_iota(jnp.int32, (height, nz * ny), 0)
    b = lax.broadcasted_iota(jnp.int32, (height, nz * ny), 1)
    pick = jnp.where(r // Q == b, 1.0, 0.0).astype(f32)
    entries = dot(pick, gd[...].reshape(nz * ny, V))
    r = lax.broadcasted_iota(jnp.int32, (height, V), 0)
    b = lax.broadcasted_iota(jnp.int32, (height, V), 1)
    entry[...] = dot(jnp.where(r % Q == b, entries, 0.0), jnp.ones((V, V), f32))
    sums.arrive()
    factor = metric_factor(rows_of(m2), work)
    Flow.ends(again)
    zs = split(jnp.concatenate([rows_of(hx), rows_of(hw)], 1))
    more = Sum(place, three(dot3(ys, zs, 0, 0)), p0, p1, p2, psem)
    more.middle()
    more.arrive()
    mix, ritz = first_mixing(factor, rows_of(p2), work)
    mixes = split(mix)
    vectors, images = dot3(ys, mixes), dot3(zs, mixes)
    vs = split(vectors)
    search, squares = correction_of(images, vs, ritz, entry[...])
    ws = split(search)
    image = dot3(both, ws)
    less[place.core] = image[:rows].reshape(nx, Q, V)
    less[1 - place.core] = image[rows:].reshape(nx, Q, V)
    rescatter = Spread(place, lambda x, core: less.at[core, x], lambda i: lessland.at[i], ts)
    us = split(images)
    gram = jnp.concatenate([dot3(a, ws, 0, 0) for a in (vs, ws, us)], 0)
    cross = Sum(place, gram, q0, q1, q2, qsem)
    nsum[...] = jnp.broadcast_to(squares, (8, V))
    norms = Spread(place, lambda x, core: nsum, lambda i: nland.at[i], ns)
    rescatter.arrive()
    total = less[place.core, place.x]
    for i in range(1, group):
        total = total + lessland[i]
    hk[place.z, place.y] = total
    last = [
        Flow(place, hk, slice(0, Q // 2), 1, (ek, fk)),
        Flow(place, hk, slice(Q // 2, Q), 0, (gk, ik)),
    ]
    for flow in last:
        flow.begin()
    cross.middle()
    Flow.relays(last)
    cross.arrive()
    mixes = split(second_mixing(rows_of(q2), ritz, work))
    pair = tuple(jnp.concatenate([a, b], 1) for a, b in zip(vs, ws))
    vectors = dot3(pair, mixes)
    vs = split(vectors)
    xs[...] = vectors
    own = pl.ds(pl.multiple_of((place.z * ny + place.y) * Q, Q), Q)
    ritz_out[...] = xs[own, :]
    norms.arrive()
    squares = nsum[...]
    for i in range(1, group):
        squares = squares + nland[i]
    norms_out[0:1, :] = jnp.sqrt(squares)[0:1, :]
    Flow.ends(last)
    ks = split(rows_of(hk))
    images = dot3(tuple(jnp.concatenate([a, b], 1) for a, b in zip(us, ks)), mixes)
    values = Sum(place, dot3(vs, split(images), 0, 0), l0, l1, l2, lsem)
    values.middle()
    values.arrive()
    search, squares = correction_of(images, vs, rows_of(l2), entry[...])
    osum[...] = jnp.broadcast_to(squares, (8, V))
    final = Spread(place, lambda x, core: osum, lambda i: oland.at[i], os)
    ss[...] = search
    search_out[...] = ss[own, :]
    Flow.drain(flows + [small] + again + last)
    for other in (scatter, sums, more, rescatter, cross, norms, values):
        other.drain()
    final.arrive()
    squares = osum[...]
    for i in range(1, group):
        squares = squares + oland[i]
    norms_out[1:2, :] = jnp.sqrt(squares)[0:1, :]
    final.drain()


def per_device(dims, kernel, ritz_block, search_block, precond_diag):
    nz, ny, _, nx = dims
    height, group, rows = nz * ny * Q, 2 * nx, nx * Q
    grid = pltpu.VMEM((nz, ny, Q, V), f32)
    entries = jnp.pad(precond_diag, (0, V - Q)).reshape(1, V)
    small = [pltpu.VMEM((8, V), f32), pltpu.VMEM((group, 8, V), f32)]
    scratch = [grid] * 5 + [
        pltpu.VMEM((nz, ny, 1, V), f32),
        pltpu.VMEM((height, V), f32),
        pltpu.VMEM((rows, 2 * height), f32),
        pltpu.VMEM((2, rows, height), f32),
        pltpu.VMEM((rows, height), f32),
        pltpu.VMEM((2, nx, Q, 2 * V), f32),
        pltpu.VMEM((group, Q, 2 * V), f32),
        pltpu.VMEM((2, nx, Q, V), f32),
        pltpu.VMEM((group, Q, V), f32),
    ]
    scratch += sum_scratch(group, 3 * V // group) * 3 + sum_scratch(group, V // group)
    scratch += small * 2 + [pltpu.VMEM((height, V), f32)] * 2 + [pltpu.VMEM((V, 2 * V), f32)]
    scratch += [pltpu.SemaphoreType.DMA((4,)), pltpu.SemaphoreType.DMA((2,))]
    for _ in range(7):
        scratch += flow_sems(dims)
    scratch += [near_sems() for _ in range(4)]
    return pl.pallas_call(
        functools.partial(davidson_kernel, dims),
        out_shape=tuple(jax.ShapeDtypeStruct(s, f32) for s in ((Q, V), (Q, V), (2, V))),
        in_specs=[pl.BlockSpec(memory_space=pl.ANY)] * 4,
        out_specs=(pl.BlockSpec(memory_space=pltpu.VMEM),) * 3,
        scratch_shapes=scratch,
        compiler_params=pltpu.CompilerParams(collective_id=0, has_side_effects=True),
    )(kernel.reshape(rows, 2 * height), ritz_block, search_block, entries)


def solution(mesh):
    chips, cols = mesh.shape["blk"] // 2, mesh.shape["col"]
    ny = min(8, chips // 2)
    dims = (chips // ny, ny, 2, cols)
    torus = Mesh(mesh.devices.reshape(dims), BLK_COL)
    placed = (P(BLK, "col", None), P(BLK_COL, None), P(BLK_COL, None), P(BLK_COL))
    return jax.shard_map(
        functools.partial(per_device, dims),
        mesh=torus,
        in_specs=placed,
        out_specs=(P(BLK_COL, None), P(BLK_COL, None), P()),
        check_vma=False,
    )
```

```python
import functools

import jax
import jax.numpy as jnp
from jax import lax
from jax.experimental import pallas as pl
from jax.experimental.pallas import tpu as pltpu
from jax.sharding import Mesh
from jax.sharding import PartitionSpec as P

MESH = pl.DeviceIdType.MESH
BLK = ("blk_0", "blk_1", "blk_2")
BLK_COL = ("blk_0", "blk_1", "blk_2", "col")
V = 128
Q = 16
PANEL = 32
f32 = jnp.float32
bf16 = jnp.bfloat16
highest = lax.Precision.HIGHEST


def dot(a, b, ca=1, cb=0):
    return lax.dot_general(
        a, b, (((ca,), (cb,)), ((), ())), precision=highest, preferred_element_type=f32
    )


def split(a):
    high = a.astype(bf16)
    return high, (a - high.astype(f32)).astype(bf16)


def dot3(a, b, ca=1, cb=0):
    dims = (((ca,), (cb,)), ((), ()))

    def one(x, y):
        return lax.dot_general(x, y, dims, preferred_element_type=f32)

    return one(a[0], b[0]) + (one(a[0], b[1]) + one(a[1], b[0]))


def inverse_factor(matrix, work):
    row = lax.broadcasted_iota(jnp.int32, (V, V), 0)
    lane = lax.broadcasted_iota(jnp.int32, (V, V), 1)
    work[:, :V] = matrix
    work[:, V:] = jnp.where(row == lane, 1.0, 0.0).astype(f32)
    sub = lax.broadcasted_iota(jnp.int32, (PANEL, V), 0)
    for start in range(0, V, PANEL):
        end = start + PANEL
        left = work[start:end, :V]
        right = work[start:end, V:]
        columns = [
            jnp.broadcast_to(left[:, start + t : start + t + 1], (PANEL, V)) for t in range(PANEL)
        ]
        scale = jnp.zeros((PANEL, V), f32)
        for r in range(PANEL):
            inverse = lax.rsqrt(jnp.broadcast_to(columns[r][r : r + 1, :], (PANEL, V)))
            scale = jnp.where(sub == r, inverse, scale)
            if r == PANEL - 1:
                break
            factor = jnp.where(sub > r, columns[r] * inverse, 0.0)
            for t in range(r + 1, PANEL):
                columns[t] = columns[t] - factor * factor[t : t + 1, :]
            factor = factor * inverse
            left = left - factor * left[r : r + 1, :]
            right = right - factor * right[r : r + 1, :]
        left = left * scale
        right = right * scale
        work[start:end, V:] = right
        if end < V:
            lower = dot(left, jnp.concatenate([left, right], 1), 0, 0)
            work[end:, :] = work[end:, :] - lower[end:, :]
    return work[:, V:]


class Place:
    def __init__(self, dims):
        self.dims = dims
        self.z, self.y, self.core, self.x = (lax.axis_index(a) for a in BLK_COL)

    def plane(self, axis, step):
        name = ("blk_0", "blk_1")[axis]
        size = self.dims[axis]
        here = (self.z, self.y)[axis]
        return {name: lax.rem(here + step + size, size)}

    def near(self, index):
        dx, dc = index // 2, index % 2
        x = lax.rem(self.x + dx, self.dims[3])
        core = lax.rem(self.core + dc, 2)
        return x, core, {"col": x, "blk_2": core}

    def group(self):
        return self.x * 2 + self.core

    def enter(self, plane):
        barrier = pltpu.get_barrier_semaphore()
        count = 0
        peers = [self.near(i)[2] for i in range(1, 2 * self.dims[3])]
        if plane:
            for axis in range(2):
                peers += [self.plane(axis, s) for s in range(1, self.dims[axis])]
        for peer in peers:
            pl.semaphore_signal(barrier, inc=1, device_id=peer, device_id_type=MESH)
            count += 1
        return barrier, count


def remote(src, dst, send, recv, to):
    return pltpu.make_async_remote_copy(
        src_ref=src,
        dst_ref=dst,
        send_sem=send,
        recv_sem=recv,
        device_id=to,
        device_id_type=MESH,
    )


class Flow:
    def __init__(self, place, buffer, rows, first, sems):
        self.place, self.buffer, self.rows, self.first = place, buffer, rows, first
        self.second = 1 - first
        self.near = Flow.steps(place.dims[first])
        self.far = Flow.steps(place.dims[self.second])[::-1]
        self.send, self.receive = sems
        self.sent = []
        here = (place.z, place.y)
        self.here, self.there = here[first], here[self.second]

    @staticmethod
    def steps(size):
        return sorted((d if d <= size // 2 else d - size for d in range(1, size)), key=abs)

    def start(self, ref, number, axis, step):
        copy = remote(
            ref,
            ref,
            self.send.at[len(self.sent)],
            self.receive.at[number],
            self.place.plane(axis, step),
        )
        copy.start()
        self.sent.append(copy)
        return copy

    def block(self, here, there):
        at = (here, there) if self.first == 0 else (there, here)
        return self.buffer.at[at[0], at[1], self.rows]

    def fan(self, here):
        for i, step in enumerate(self.far):
            self.start(self.block(here, self.there), len(self.near) + i, self.second, step)

    def begin(self):
        own = self.block(self.here, self.there)
        self.first_copies = [
            self.start(own, i, self.first, step) for i, step in enumerate(self.near)
        ]
        self.fan(self.here)

    def relay(self, i):
        self.first_copies[i].wait_recv()
        size = self.place.dims[self.first]
        self.fan(lax.rem(self.here - self.near[i] + size, size))

    def end(self):
        size = self.place.dims[self.second]
        for i, step in enumerate(self.far):
            origin = lax.rem(self.there - step + size, size)
            if self.first == 0:
                line = self.buffer.at[:, origin, self.rows]
            else:
                line = self.buffer.at[origin, :, self.rows]
            number = len(self.near) + i
            remote(
                line,
                line,
                self.send.at[0],
                self.receive.at[number],
                self.place.plane(self.second, step),
            ).wait_recv()

    @staticmethod
    def relays(flows):
        for i in range(max(len(f.near) for f in flows)):
            for flow in flows:
                if i < len(flow.near):
                    flow.relay(i)

    @staticmethod
    def ends(flows):
        for flow in flows:
            flow.end()

    @staticmethod
    def drain(flows):
        for flow in flows:
            for copy in flow.sent:
                copy.wait_send()


class Lines:
    def __init__(self, place, buffer, send, receive):
        self.place, self.buffer, self.send, self.receive = place, buffer, send, receive
        self.copies = []
        self.start(buffer.at[place.z, place.y], 1)

    def start(self, ref, axis):
        at = len(self.copies)
        for i, step in enumerate(Flow.steps(self.place.dims[axis])):
            peer = self.place.plane(axis, step)
            copy = remote(ref, ref, self.send.at[at + i], self.receive.at[at + i], peer)
            copy.start()
            self.copies.append(copy)
        self.pending = self.copies[at:]

    def middle(self):
        self.arrive()
        self.start(self.buffer.at[self.place.z], 0)

    def arrive(self):
        for copy in self.pending:
            copy.wait_recv()

    def drain(self):
        for copy in self.copies:
            copy.wait_send()


def flow_sems(dims):
    nz, ny = dims[:2]
    return [
        pltpu.SemaphoreType.DMA((nz * ny + max(nz, ny),)),
        pltpu.SemaphoreType.DMA((nz + ny,)),
    ]


class Spread:
    def __init__(self, place, source, target, sems):
        self.place = place
        self.copies = []
        for i in range(1, 2 * place.dims[3]):
            x, core, to = place.near(i)
            self.copies.append(
                remote(source(x, core), target(i), sems.at[0, i], sems.at[1, i], to)
            )
        for copy in self.copies:
            copy.start()

    def arrive(self):
        for copy in self.copies:
            copy.wait_recv()

    def drain(self):
        for copy in self.copies:
            copy.wait_send()


class Sum:
    def __init__(self, place, value, pieces, landed, whole, sems):
        self.place, self.pieces, self.landed, self.whole = place, pieces, landed, whole
        self.sems = sems
        pieces[...] = value.reshape(pieces.shape)
        self.scatter = Spread(
            place, lambda x, core: pieces.at[x * 2 + core], lambda i: landed.at[i], sems.at[0]
        )

    def middle(self):
        place, own = self.place, self.place.group()
        self.scatter.arrive()
        total = self.pieces[own]
        for i in range(1, 2 * place.dims[3]):
            total = total + self.landed[i]
        self.whole[own] = total
        self.share = Spread(
            place,
            lambda x, core: self.whole.at[own],
            lambda i: self.whole.at[own],
            self.sems.at[1],
        )

    def arrive(self):
        self.share.arrive()

    def drain(self):
        self.scatter.drain()
        self.share.drain()


def near_sems(*lead):
    return pltpu.SemaphoreType.DMA((*lead, 2, 8))


def sum_scratch(group, rows):
    return [pltpu.VMEM((group, rows, V), f32)] * 3 + [near_sems(2)]


def rows_of(buffer):
    return buffer[...].reshape(-1, buffer.shape[-1])


def three(gram):
    return jnp.concatenate([gram[:V, :V], gram[:V, V:], gram[V:, V:]], 0)


def metric_factor(metric, work):
    xx, xw, ww = (metric[i * V : (i + 1) * V, :] for i in range(3))
    top = inverse_factor(xx, work)
    side = dot(top, xw)
    low = inverse_factor(ww - dot(side, side, 0, 0), work)
    cross = -dot(dot(low, side, 1, 1), top)
    zero = jnp.zeros((V, V), f32)
    return jnp.concatenate(
        [jnp.concatenate([top, zero], 1), jnp.concatenate([cross, low], 1)], 0
    )


def first_mixing(factor, projected, rest, work):
    xx, xw = projected[:V, :], projected[V:, :]
    left = jnp.concatenate([xx, xw.T], 0)
    half = dot(factor, left)
    power = dot(factor, half, 0, 0)
    rest.middle()
    back = inverse_factor(dot(half, half, 0, 0), work)
    rest.arrive()
    whole = jnp.concatenate([left, jnp.concatenate([xw, rows_of(rest.whole)], 0)], 1)
    mix = dot(power, back, 1, 1)
    return mix, dot(mix, dot(whole, mix), 0, 0)


def second_mixing(sums, ritz, work):
    xw, ww, image = (sums[i * V : (i + 1) * V, :] for i in range(3))
    low = inverse_factor(ww - dot(xw, xw, 0, 0), work)
    lower = dot(low, image.T - dot(xw, ritz, 0, 0))
    back = inverse_factor(dot(ritz, ritz, 0, 0) + dot(lower, lower, 0, 0), work)
    lower = dot(low, dot(lower, back, 1, 1), 0, 0)
    upper = dot(ritz, back, 1, 1) - dot(xw, lower)
    return jnp.concatenate([upper, lower], 0)


def correction_of(images, moved, ritz, diag):
    row = lax.broadcasted_iota(jnp.int32, (V, V), 0)
    lane = lax.broadcasted_iota(jnp.int32, (V, V), 1)
    values = jnp.sum(jnp.where(row == lane, ritz, 0.0), axis=0, keepdims=True)
    residual = images - moved
    squares = jnp.sum(residual * residual, axis=0, keepdims=True)
    return residual / jnp.maximum(jnp.abs(diag - values), 1.0), squares


def davidson_kernel(
    dims, k_in, x_in, w_in, d_in, ritz_out, search_out, norms_out,
    gx, gw, hx, hw, hk, gd, dsm, entry, kraw, kown, kland, part, landed, less, lessland,
    m0, m1, m2, msem, p0, p1, p2, psem, r0, r1, r2, rsem, q0, q1, q2, qsem, l0, l1, l2, lsem,
    nsum, nland, osum, oland, xs, ss, work,
    load, ksem, ax, bx, aw, bw, cx, dx, cw, dw, ek, fk, gk, ik, ad, bd, rs, ts, ns, os,
):
    place = Place(dims)
    nz, ny, _, nx = dims
    group = 2 * nx
    barrier, count = place.enter(True)
    taps = pltpu.make_async_copy(d_in, dsm, load.at[2])
    loads = [
        pltpu.make_async_copy(x_in, gx.at[place.z, place.y], load.at[0]),
        pltpu.make_async_copy(w_in, gw.at[place.z, place.y], load.at[1]),
        taps,
        pltpu.make_async_copy(k_in.at[:, 0], kraw, load.at[3]),
    ]
    for copy in loads:
        copy.start()
    for copy in loads[:3]:
        copy.wait()
    pl.semaphore_wait(barrier, count)
    flows = [
        Flow(place, gx, slice(None), 1, (ax, bx)),
        Flow(place, gw, slice(None), 0, (aw, bw)),
    ]
    for flow in flows:
        flow.begin()
    lane = lax.broadcasted_iota(jnp.int32, (1, V), 1)
    line = jnp.zeros((1, V), f32)
    for k in range(Q):
        line = jnp.where(lane == k, dsm[k], line)
    gd[place.z, place.y] = line
    Flow.relays(flows)
    loads[3].wait()
    i = lax.broadcasted_iota(jnp.int32, (2 * V, 2 * V), 0)
    j = lax.broadcasted_iota(jnp.int32, (2 * V, 2 * V), 1)
    to = ((i // Q) % 2) * V + (i // (2 * Q)) * Q + i % Q
    mover = jnp.where(j == to, 1.0, 0.0).astype(f32)
    for tile in range(kraw.shape[1] // (2 * V)):
        moved = dot(kraw[:, tile * 2 * V : (tile + 1) * 2 * V], mover)
        kown[0, :, tile * V : (tile + 1) * V] = moved[:, :V]
        kown[1, :, tile * V : (tile + 1) * V] = moved[:, V:]
    swap = remote(kown.at[1 - place.core], kland, ksem.at[0], ksem.at[1], place.near(1)[2])
    swap.start()
    swap.wait()
    both = split(jnp.concatenate([kown[place.core], kland[...]], 0))
    rows = kland.shape[0]
    Flow.ends(flows)
    ys = split(jnp.concatenate([rows_of(gx), rows_of(gw)], 1))
    image = dot3(both, ys)
    part[place.core] = image[:rows].reshape(nx, Q, 2 * V)
    part[1 - place.core] = image[rows:].reshape(nx, Q, 2 * V)
    scatter = Spread(place, lambda x, core: part.at[core, x], lambda i: landed.at[i], rs)
    small = Lines(place, gd, ad, bd)
    sums = Sum(place, three(dot3(ys, ys, 0, 0)), m0, m1, m2, msem)
    scatter.arrive()
    total = part[place.core, place.x]
    for i in range(1, group):
        total = total + landed[i]
    hx[place.z, place.y] = total[:, :V]
    hw[place.z, place.y] = total[:, V:]
    again = [
        Flow(place, hx, slice(None), 1, (cx, dx)),
        Flow(place, hw, slice(None), 0, (cw, dw)),
    ]
    for flow in again:
        flow.begin()
    sums.middle()
    Flow.relays(again)
    small.middle()
    sums.arrive()
    factor = metric_factor(rows_of(m2), work)
    small.arrive()
    height = nz * ny * Q
    r = lax.broadcasted_iota(jnp.int32, (height, nz * ny), 0)
    b = lax.broadcasted_iota(jnp.int32, (height, nz * ny), 1)
    pick = jnp.where(r // Q == b, 1.0, 0.0).astype(f32)
    entries = dot(pick, gd[...].reshape(nz * ny, V))
    r = lax.broadcasted_iota(jnp.int32, (height, V), 0)
    b = lax.broadcasted_iota(jnp.int32, (height, V), 1)
    entry[...] = dot(jnp.where(r % Q == b, entries, 0.0), jnp.ones((V, V), f32))
    Flow.ends(again)
    zs = split(jnp.concatenate([rows_of(hx), rows_of(hw)], 1))
    gram = three(dot3(ys, zs, 0, 0))
    more = Sum(place, gram[: 2 * V], p0, p1, p2, psem)
    rest = Sum(place, gram[2 * V :], r0, r1, r2, rsem)
    more.middle()
    more.arrive()
    mix, ritz = first_mixing(factor, rows_of(p2), rest, work)
    mixes = split(mix)
    images = dot3(zs, mixes)
    moved = dot3(ys, split(dot(mix, ritz)))
    search, squares = correction_of(images, moved, ritz, entry[...])
    ws = split(search)
    image = dot3(both, ws)
    less[place.core] = image[:rows].reshape(nx, Q, V)
    less[1 - place.core] = image[rows:].reshape(nx, Q, V)
    rescatter = Spread(place, lambda x, core: less.at[core, x], lambda i: lessland.at[i], ts)
    vs, us = split(dot3(ys, mixes)), split(images)
    gram = jnp.concatenate([dot3(a, ws, 0, 0) for a in (vs, ws, us)], 0)
    cross = Sum(place, gram, q0, q1, q2, qsem)
    nsum[...] = jnp.broadcast_to(squares, (8, V))
    norms = Spread(place, lambda x, core: nsum, lambda i: nland.at[i], ns)
    rescatter.arrive()
    total = less[place.core, place.x]
    for i in range(1, group):
        total = total + lessland[i]
    hk[place.z, place.y] = total
    last = [
        Flow(place, hk, slice(0, Q // 2), 1, (ek, fk)),
        Flow(place, hk, slice(Q // 2, Q), 0, (gk, ik)),
    ]
    for flow in last:
        flow.begin()
    cross.middle()
    Flow.relays(last)
    cross.arrive()
    mixes = split(second_mixing(rows_of(q2), ritz, work))
    pair = tuple(jnp.concatenate([a, b], 1) for a, b in zip(vs, ws))
    vectors = dot3(pair, mixes)
    vs = split(vectors)
    xs[...] = vectors
    own = pl.ds(pl.multiple_of((place.z * ny + place.y) * Q, Q), Q)
    ritz_out[...] = xs[own, :]
    norms.arrive()
    squares = nsum[...]
    for i in range(1, group):
        squares = squares + nland[i]
    norms_out[0:1, :] = jnp.sqrt(squares)[0:1, :]
    Flow.ends(last)
    ks = split(rows_of(hk))
    images = dot3(tuple(jnp.concatenate([a, b], 1) for a, b in zip(us, ks)), mixes)
    values = Sum(place, dot3(vs, split(images), 0, 0), l0, l1, l2, lsem)
    values.middle()
    values.arrive()
    ritz = rows_of(l2)
    search, squares = correction_of(images, dot3(vs, split(ritz)), ritz, entry[...])
    osum[...] = jnp.broadcast_to(squares, (8, V))
    final = Spread(place, lambda x, core: osum, lambda i: oland.at[i], os)
    ss[...] = search
    search_out[...] = ss[own, :]
    Flow.drain(flows + again + last)
    for other in (small, scatter, sums, more, rest, rescatter, cross, norms, values):
        other.drain()
    final.arrive()
    squares = osum[...]
    for i in range(1, group):
        squares = squares + oland[i]
    norms_out[1:2, :] = jnp.sqrt(squares)[0:1, :]
    final.drain()


def per_device(dims, kernel, ritz_block, search_block, precond_diag):
    nz, ny, _, nx = dims
    height, group, rows = nz * ny * Q, 2 * nx, nx * Q
    grid = pltpu.VMEM((nz, ny, Q, V), f32)
    small = [pltpu.VMEM((8, V), f32), pltpu.VMEM((group, 8, V), f32)]
    scratch = [grid] * 5 + [
        pltpu.VMEM((nz, ny, 1, V), f32),
        pltpu.SMEM((Q,), f32),
        pltpu.VMEM((height, V), f32),
        pltpu.VMEM((rows, 2 * height), f32),
        pltpu.VMEM((2, rows, height), f32),
        pltpu.VMEM((rows, height), f32),
        pltpu.VMEM((2, nx, Q, 2 * V), f32),
        pltpu.VMEM((group, Q, 2 * V), f32),
        pltpu.VMEM((2, nx, Q, V), f32),
        pltpu.VMEM((group, Q, V), f32),
    ]
    for height_of in (3, 2, 1, 3, 1):
        scratch += sum_scratch(group, height_of * V // group)
    scratch += small * 2 + [pltpu.VMEM((height, V), f32)] * 2 + [pltpu.VMEM((V, 2 * V), f32)]
    scratch += [pltpu.SemaphoreType.DMA((4,)), pltpu.SemaphoreType.DMA((2,))]
    for _ in range(6):
        scratch += flow_sems(dims)
    scratch += [pltpu.SemaphoreType.DMA((nz + ny,))] * 2
    scratch += [near_sems() for _ in range(4)]
    return pl.pallas_call(
        functools.partial(davidson_kernel, dims),
        out_shape=tuple(jax.ShapeDtypeStruct(s, f32) for s in ((Q, V), (Q, V), (2, V))),
        in_specs=[pl.BlockSpec(memory_space=pl.ANY)] * 4,
        out_specs=(pl.BlockSpec(memory_space=pltpu.VMEM),) * 3,
        scratch_shapes=scratch,
        compiler_params=pltpu.CompilerParams(collective_id=0, has_side_effects=True),
    )(kernel, ritz_block, search_block, precond_diag)


def solution(mesh):
    chips, cols = mesh.shape["blk"] // 2, mesh.shape["col"]
    ny = min(8, chips // 2)
    dims = (chips // ny, ny, 2, cols)
    torus = Mesh(mesh.devices.reshape(dims), BLK_COL)
    placed = (P(BLK, "col", None), P(BLK_COL, None), P(BLK_COL, None), P(BLK_COL))
    return jax.shard_map(
        functools.partial(per_device, dims),
        mesh=torus,
        in_specs=placed,
        out_specs=(P(BLK_COL, None), P(BLK_COL, None), P()),
        check_vma=False,
    )
```

```python
import functools

import jax
import jax.numpy as jnp
from jax import lax
from jax.experimental import pallas as pl
from jax.experimental.pallas import tpu as pltpu
from jax.sharding import Mesh
from jax.sharding import PartitionSpec as P

MESH = pl.DeviceIdType.MESH
BLK = ("blk_0", "blk_1", "blk_2")
BLK_COL = ("blk_0", "blk_1", "blk_2", "col")
V = 128
Q = 16
PANEL = 32
f32 = jnp.float32
bf16 = jnp.bfloat16
highest = lax.Precision.HIGHEST


def dot(a, b, ca=1, cb=0):
    return lax.dot_general(
        a, b, (((ca,), (cb,)), ((), ())), precision=highest, preferred_element_type=f32
    )


def split(a):
    high = a.astype(bf16)
    return high, (a - high.astype(f32)).astype(bf16)


def dot3(a, b, ca=1, cb=0):
    dims = (((ca,), (cb,)), ((), ()))

    def one(x, y):
        return lax.dot_general(x, y, dims, preferred_element_type=f32)

    return one(a[0], b[0]) + (one(a[0], b[1]) + one(a[1], b[0]))


def inverse_factor(matrix, work):
    row = lax.broadcasted_iota(jnp.int32, (V, V), 0)
    lane = lax.broadcasted_iota(jnp.int32, (V, V), 1)
    work[:, :V] = matrix
    work[:, V:] = jnp.where(row == lane, 1.0, 0.0).astype(f32)
    sub = lax.broadcasted_iota(jnp.int32, (PANEL, V), 0)
    for start in range(0, V, PANEL):
        end = start + PANEL
        left = work[start:end, :V]
        right = work[start:end, V:]
        columns = [
            jnp.broadcast_to(left[:, start + t : start + t + 1], (PANEL, V)) for t in range(PANEL)
        ]
        scale = jnp.zeros((PANEL, V), f32)
        for r in range(PANEL):
            inverse = lax.rsqrt(jnp.broadcast_to(columns[r][r : r + 1, :], (PANEL, V)))
            scale = jnp.where(sub == r, inverse, scale)
            if r == PANEL - 1:
                break
            factor = jnp.where(sub > r, columns[r] * inverse, 0.0)
            for t in range(r + 1, PANEL):
                columns[t] = columns[t] - factor * factor[t : t + 1, :]
            factor = factor * inverse
            left = left - factor * left[r : r + 1, :]
            right = right - factor * right[r : r + 1, :]
        left = left * scale
        right = right * scale
        work[start:end, V:] = right
        if end < V:
            lower = dot(left, jnp.concatenate([left, right], 1), 0, 0)
            work[end:, :] = work[end:, :] - lower[end:, :]
    return work[:, V:]


class Place:
    def __init__(self, dims):
        self.dims = dims
        self.z, self.y, self.core, self.x = (lax.axis_index(a) for a in BLK_COL)

    def plane(self, axis, step):
        name = ("blk_0", "blk_1")[axis]
        size = self.dims[axis]
        here = (self.z, self.y)[axis]
        return {name: lax.rem(here + step + size, size)}

    def near(self, index):
        dx, dc = index // 2, index % 2
        x = lax.rem(self.x + dx, self.dims[3])
        core = lax.rem(self.core + dc, 2)
        return x, core, {"col": x, "blk_2": core}

    def group(self):
        return self.x * 2 + self.core

    def enter(self, plane):
        barrier = pltpu.get_barrier_semaphore()
        count = 0
        peers = [self.near(i)[2] for i in range(1, 2 * self.dims[3])]
        if plane:
            for axis in range(2):
                peers += [self.plane(axis, s) for s in range(1, self.dims[axis])]
        for peer in peers:
            pl.semaphore_signal(barrier, inc=1, device_id=peer, device_id_type=MESH)
            count += 1
        return barrier, count


def remote(src, dst, send, recv, to):
    return pltpu.make_async_remote_copy(
        src_ref=src,
        dst_ref=dst,
        send_sem=send,
        recv_sem=recv,
        device_id=to,
        device_id_type=MESH,
    )


class Flow:
    def __init__(self, place, buffer, rows, first, sems):
        self.place, self.buffer, self.rows, self.first = place, buffer, rows, first
        self.second = 1 - first
        self.near = Flow.steps(place.dims[first])
        self.far = Flow.steps(place.dims[self.second])[::-1]
        self.send, self.receive = sems
        self.sent = []
        here = (place.z, place.y)
        self.here, self.there = here[first], here[self.second]

    @staticmethod
    def steps(size):
        return sorted((d if d <= size // 2 else d - size for d in range(1, size)), key=abs)

    def start(self, ref, number, axis, step):
        copy = remote(
            ref,
            ref,
            self.send.at[len(self.sent)],
            self.receive.at[number],
            self.place.plane(axis, step),
        )
        copy.start()
        self.sent.append(copy)
        return copy

    def block(self, here, there):
        at = (here, there) if self.first == 0 else (there, here)
        return self.buffer.at[at[0], at[1], self.rows]

    def fan(self, here):
        for i, step in enumerate(self.far):
            self.start(self.block(here, self.there), len(self.near) + i, self.second, step)

    def begin(self):
        own = self.block(self.here, self.there)
        self.first_copies = [
            self.start(own, i, self.first, step) for i, step in enumerate(self.near)
        ]
        self.fan(self.here)

    def relay(self, i):
        self.first_copies[i].wait_recv()
        size = self.place.dims[self.first]
        self.fan(lax.rem(self.here - self.near[i] + size, size))

    def end(self):
        size = self.place.dims[self.second]
        for i, step in enumerate(self.far):
            origin = lax.rem(self.there - step + size, size)
            if self.first == 0:
                line = self.buffer.at[:, origin, self.rows]
            else:
                line = self.buffer.at[origin, :, self.rows]
            number = len(self.near) + i
            remote(
                line,
                line,
                self.send.at[0],
                self.receive.at[number],
                self.place.plane(self.second, step),
            ).wait_recv()

    @staticmethod
    def relays(flows):
        for i in range(max(len(f.near) for f in flows)):
            for flow in flows:
                if i < len(flow.near):
                    flow.relay(i)

    @staticmethod
    def ends(flows):
        for flow in flows:
            flow.end()

    @staticmethod
    def drain(flows):
        for flow in flows:
            for copy in flow.sent:
                copy.wait_send()


class Lines:
    def __init__(self, place, buffer, send, receive):
        self.place, self.buffer, self.send, self.receive = place, buffer, send, receive
        self.copies = []
        self.start(buffer.at[place.z, place.y], 1)

    def start(self, ref, axis):
        at = len(self.copies)
        for i, step in enumerate(Flow.steps(self.place.dims[axis])):
            peer = self.place.plane(axis, step)
            copy = remote(ref, ref, self.send.at[at + i], self.receive.at[at + i], peer)
            copy.start()
            self.copies.append(copy)
        self.pending = self.copies[at:]

    def middle(self):
        self.arrive()
        self.start(self.buffer.at[self.place.z], 0)

    def arrive(self):
        for copy in self.pending:
            copy.wait_recv()

    def drain(self):
        for copy in self.copies:
            copy.wait_send()


def flow_sems(dims):
    nz, ny = dims[:2]
    return [
        pltpu.SemaphoreType.DMA((nz * ny + max(nz, ny),)),
        pltpu.SemaphoreType.DMA((nz + ny,)),
    ]


class Spread:
    def __init__(self, place, source, target, sems):
        self.place = place
        self.copies = []
        size = place.dims[3]
        for i in sorted(range(1, 2 * size), key=lambda i: -min(i // 2, size - i // 2)):
            x, core, to = place.near(i)
            self.copies.append(
                remote(source(x, core), target(i), sems.at[0, i], sems.at[1, i], to)
            )
        for copy in self.copies:
            copy.start()

    def arrive(self):
        for copy in self.copies:
            copy.wait_recv()

    def drain(self):
        for copy in self.copies:
            copy.wait_send()


class Sum:
    def __init__(self, place, value, pieces, landed, whole, sems):
        self.place, self.pieces, self.landed, self.whole = place, pieces, landed, whole
        self.sems = sems
        pieces[...] = value.reshape(pieces.shape)
        self.scatter = Spread(
            place, lambda x, core: pieces.at[x * 2 + core], lambda i: landed.at[i], sems.at[0]
        )

    def middle(self):
        place, own = self.place, self.place.group()
        self.scatter.arrive()
        total = self.pieces[own]
        for i in range(1, 2 * place.dims[3]):
            total = total + self.landed[i]
        self.whole[own] = total
        self.share = Spread(
            place,
            lambda x, core: self.whole.at[own],
            lambda i: self.whole.at[own],
            self.sems.at[1],
        )

    def arrive(self):
        self.share.arrive()

    def drain(self):
        self.scatter.drain()
        self.share.drain()


def near_sems(*lead):
    return pltpu.SemaphoreType.DMA((*lead, 2, 8))


def sum_scratch(group, rows):
    return [pltpu.VMEM((group, rows, V), f32)] * 3 + [near_sems(2)]


def rows_of(buffer):
    return buffer[...].reshape(-1, buffer.shape[-1])


def three(gram):
    return jnp.concatenate([gram[:V, :V], gram[:V, V:], gram[V:, V:]], 0)


def metric_factor(metric, work):
    xx, xw, ww = (metric[i * V : (i + 1) * V, :] for i in range(3))
    top = inverse_factor(xx, work)
    side = dot(top, xw)
    low = inverse_factor(ww - dot(side, side, 0, 0), work)
    cross = -dot(dot(low, side, 1, 1), top)
    zero = jnp.zeros((V, V), f32)
    return jnp.concatenate(
        [jnp.concatenate([top, zero], 1), jnp.concatenate([cross, low], 1)], 0
    )


def first_mixing(factor, projected, rest, work):
    xx, xw = projected[:V, :], projected[V:, :]
    left = jnp.concatenate([xx, xw.T], 0)
    half = dot(factor, left)
    power = dot(factor, half, 0, 0)
    rest.middle()
    back = inverse_factor(dot(half, half, 0, 0), work)
    rest.arrive()
    whole = jnp.concatenate([left, jnp.concatenate([xw, rows_of(rest.whole)], 0)], 1)
    mix = dot(power, back, 1, 1)
    return mix, dot(mix, dot(whole, mix), 0, 0)


def second_mixing(sums, ritz, work):
    xw, ww, image = (sums[i * V : (i + 1) * V, :] for i in range(3))
    low = inverse_factor(ww - dot(xw, xw, 0, 0), work)
    lower = dot(low, image.T - dot(xw, ritz, 0, 0))
    back = inverse_factor(dot(ritz, ritz, 0, 0) + dot(lower, lower, 0, 0), work)
    lower = dot(low, dot(lower, back, 1, 1), 0, 0)
    upper = dot(ritz, back, 1, 1) - dot(xw, lower)
    return jnp.concatenate([upper, lower], 0)


def correction_of(images, moved, ritz, diag):
    row = lax.broadcasted_iota(jnp.int32, (V, V), 0)
    lane = lax.broadcasted_iota(jnp.int32, (V, V), 1)
    values = jnp.sum(jnp.where(row == lane, ritz, 0.0), axis=0, keepdims=True)
    residual = images - moved
    squares = jnp.sum(residual * residual, axis=0, keepdims=True)
    return residual / jnp.maximum(jnp.abs(diag - values), 1.0), squares


def davidson_kernel(
    dims, k_in, x_in, w_in, d_in, ritz_out, search_out, norms_out,
    gx, gw, hx, hw, hk, gd, dsm, entry, kraw, kown, kland, part, landed, less, lessland,
    m0, m1, m2, msem, p0, p1, p2, psem, r0, r1, r2, rsem, q0, q1, q2, qsem, l0, l1, l2, lsem,
    nsum, nland, osum, oland, xs, ss, work,
    load, ksem, ax, bx, aw, bw, cx, dx, cw, dw, ek, fk, gk, ik, ad, bd, rs, ts, ns, os,
):
    place = Place(dims)
    nz, ny, _, nx = dims
    group = 2 * nx
    barrier, count = place.enter(True)
    taps = pltpu.make_async_copy(d_in, dsm, load.at[2])
    loads = [
        pltpu.make_async_copy(x_in, gx.at[place.z, place.y], load.at[0]),
        pltpu.make_async_copy(w_in, gw.at[place.z, place.y], load.at[1]),
        taps,
        pltpu.make_async_copy(k_in.at[:, 0], kraw, load.at[3]),
    ]
    for copy in loads:
        copy.start()
    for copy in loads[:3]:
        copy.wait()
    pl.semaphore_wait(barrier, count)
    flows = [
        Flow(place, gx, slice(None), 1, (ax, bx)),
        Flow(place, gw, slice(None), 0, (aw, bw)),
    ]
    for flow in flows:
        flow.begin()
    lane = lax.broadcasted_iota(jnp.int32, (1, V), 1)
    line = jnp.zeros((1, V), f32)
    for k in range(Q):
        line = jnp.where(lane == k, dsm[k], line)
    gd[place.z, place.y] = line
    Flow.relays(flows)
    loads[3].wait()
    i = lax.broadcasted_iota(jnp.int32, (2 * V, 2 * V), 0)
    j = lax.broadcasted_iota(jnp.int32, (2 * V, 2 * V), 1)
    to = ((i // Q) % 2) * V + (i // (2 * Q)) * Q + i % Q
    mover = jnp.where(j == to, 1.0, 0.0).astype(f32)
    for tile in range(kraw.shape[1] // (2 * V)):
        moved = dot(kraw[:, tile * 2 * V : (tile + 1) * 2 * V], mover)
        kown[0, :, tile * V : (tile + 1) * V] = moved[:, :V]
        kown[1, :, tile * V : (tile + 1) * V] = moved[:, V:]
    swap = remote(kown.at[1 - place.core], kland, ksem.at[0], ksem.at[1], place.near(1)[2])
    swap.start()
    swap.wait()
    both = split(jnp.concatenate([kown[place.core], kland[...]], 0))
    rows = kland.shape[0]
    Flow.ends(flows)
    ys = split(jnp.concatenate([rows_of(gx), rows_of(gw)], 1))
    image = dot3(both, ys)
    part[place.core] = image[:rows].reshape(nx, Q, 2 * V)
    part[1 - place.core] = image[rows:].reshape(nx, Q, 2 * V)
    scatter = Spread(place, lambda x, core: part.at[core, x], lambda i: landed.at[i], rs)
    small = Lines(place, gd, ad, bd)
    sums = Sum(place, three(dot3(ys, ys, 0, 0)), m0, m1, m2, msem)
    scatter.arrive()
    total = part[place.core, place.x]
    for i in range(1, group):
        total = total + landed[i]
    hx[place.z, place.y] = total[:, :V]
    hw[place.z, place.y] = total[:, V:]
    again = [
        Flow(place, hx, slice(None), 1, (cx, dx)),
        Flow(place, hw, slice(None), 0, (cw, dw)),
    ]
    for flow in again:
        flow.begin()
    sums.middle()
    Flow.relays(again)
    small.middle()
    sums.arrive()
    factor = metric_factor(rows_of(m2), work)
    Flow.ends(again)
    zs = split(jnp.concatenate([rows_of(hx), rows_of(hw)], 1))
    gram = three(dot3(ys, zs, 0, 0))
    more = Sum(place, gram[: 2 * V], p0, p1, p2, psem)
    rest = Sum(place, gram[2 * V :], r0, r1, r2, rsem)
    small.arrive()
    height = nz * ny * Q
    r = lax.broadcasted_iota(jnp.int32, (height, nz * ny), 0)
    b = lax.broadcasted_iota(jnp.int32, (height, nz * ny), 1)
    pick = jnp.where(r // Q == b, 1.0, 0.0).astype(f32)
    entries = dot(pick, gd[...].reshape(nz * ny, V))
    r = lax.broadcasted_iota(jnp.int32, (height, V), 0)
    b = lax.broadcasted_iota(jnp.int32, (height, V), 1)
    entry[...] = dot(jnp.where(r % Q == b, entries, 0.0), jnp.ones((V, V), f32))
    more.middle()
    more.arrive()
    mix, ritz = first_mixing(factor, rows_of(p2), rest, work)
    mixes = split(mix)
    images = dot3(zs, mixes)
    moved = dot3(ys, split(dot(mix, ritz)))
    search, squares = correction_of(images, moved, ritz, entry[...])
    ws = split(search)
    image = dot3(both, ws)
    less[place.core] = image[:rows].reshape(nx, Q, V)
    less[1 - place.core] = image[rows:].reshape(nx, Q, V)
    rescatter = Spread(place, lambda x, core: less.at[core, x], lambda i: lessland.at[i], ts)
    vs, us = split(dot3(ys, mixes)), split(images)
    gram = jnp.concatenate([dot3(a, ws, 0, 0) for a in (vs, ws, us)], 0)
    cross = Sum(place, gram, q0, q1, q2, qsem)
    nsum[...] = jnp.broadcast_to(squares, (8, V))
    norms = Spread(place, lambda x, core: nsum, lambda i: nland.at[i], ns)
    rescatter.arrive()
    total = less[place.core, place.x]
    for i in range(1, group):
        total = total + lessland[i]
    hk[place.z, place.y] = total
    last = [
        Flow(place, hk, slice(0, Q // 2), 1, (ek, fk)),
        Flow(place, hk, slice(Q // 2, Q), 0, (gk, ik)),
    ]
    for flow in last:
        flow.begin()
    cross.middle()
    Flow.relays(last)
    cross.arrive()
    mixes = split(second_mixing(rows_of(q2), ritz, work))
    pair = tuple(jnp.concatenate([a, b], 1) for a, b in zip(vs, ws))
    vectors = dot3(pair, mixes)
    vs = split(vectors)
    xs[...] = vectors
    own = pl.ds(pl.multiple_of((place.z * ny + place.y) * Q, Q), Q)
    ritz_out[...] = xs[own, :]
    norms.arrive()
    squares = nsum[...]
    for i in range(1, group):
        squares = squares + nland[i]
    norms_out[0:1, :] = jnp.sqrt(squares)[0:1, :]
    Flow.ends(last)
    ks = split(rows_of(hk))
    images = dot3(tuple(jnp.concatenate([a, b], 1) for a, b in zip(us, ks)), mixes)
    values = Sum(place, dot3(vs, split(images), 0, 0), l0, l1, l2, lsem)
    values.middle()
    values.arrive()
    ritz = rows_of(l2)
    search, squares = correction_of(images, dot3(vs, split(ritz)), ritz, entry[...])
    osum[...] = jnp.broadcast_to(squares, (8, V))
    final = Spread(place, lambda x, core: osum, lambda i: oland.at[i], os)
    ss[...] = search
    search_out[...] = ss[own, :]
    Flow.drain(flows + again + last)
    for other in (small, scatter, sums, more, rest, rescatter, cross, norms, values):
        other.drain()
    final.arrive()
    squares = osum[...]
    for i in range(1, group):
        squares = squares + oland[i]
    norms_out[1:2, :] = jnp.sqrt(squares)[0:1, :]
    final.drain()


def per_device(dims, kernel, ritz_block, search_block, precond_diag):
    nz, ny, _, nx = dims
    height, group, rows = nz * ny * Q, 2 * nx, nx * Q
    grid = pltpu.VMEM((nz, ny, Q, V), f32)
    small = [pltpu.VMEM((8, V), f32), pltpu.VMEM((group, 8, V), f32)]
    scratch = [grid] * 5 + [
        pltpu.VMEM((nz, ny, 1, V), f32),
        pltpu.SMEM((Q,), f32),
        pltpu.VMEM((height, V), f32),
        pltpu.VMEM((rows, 2 * height), f32),
        pltpu.VMEM((2, rows, height), f32),
        pltpu.VMEM((rows, height), f32),
        pltpu.VMEM((2, nx, Q, 2 * V), f32),
        pltpu.VMEM((group, Q, 2 * V), f32),
        pltpu.VMEM((2, nx, Q, V), f32),
        pltpu.VMEM((group, Q, V), f32),
    ]
    for height_of in (3, 2, 1, 3, 1):
        scratch += sum_scratch(group, height_of * V // group)
    scratch += small * 2 + [pltpu.VMEM((height, V), f32)] * 2 + [pltpu.VMEM((V, 2 * V), f32)]
    scratch += [pltpu.SemaphoreType.DMA((4,)), pltpu.SemaphoreType.DMA((2,))]
    for _ in range(6):
        scratch += flow_sems(dims)
    scratch += [pltpu.SemaphoreType.DMA((nz + ny,))] * 2
    scratch += [near_sems() for _ in range(4)]
    return pl.pallas_call(
        functools.partial(davidson_kernel, dims),
        out_shape=tuple(jax.ShapeDtypeStruct(s, f32) for s in ((Q, V), (Q, V), (2, V))),
        in_specs=[pl.BlockSpec(memory_space=pl.ANY)] * 4,
        out_specs=(pl.BlockSpec(memory_space=pltpu.VMEM),) * 3,
        scratch_shapes=scratch,
        compiler_params=pltpu.CompilerParams(collective_id=0, has_side_effects=True),
    )(kernel, ritz_block, search_block, precond_diag)


def solution(mesh):
    chips, cols = mesh.shape["blk"] // 2, mesh.shape["col"]
    ny = min(8, chips // 2)
    dims = (chips // ny, ny, 2, cols)
    torus = Mesh(mesh.devices.reshape(dims), BLK_COL)
    placed = (P(BLK, "col", None), P(BLK_COL, None), P(BLK_COL, None), P(BLK_COL))
    return jax.shard_map(
        functools.partial(per_device, dims),
        mesh=torus,
        in_specs=placed,
        out_specs=(P(BLK_COL, None), P(BLK_COL, None), P()),
        check_vma=False,
    )
```
